32 devices in a mesh: comp: 8 (over z, y), band: 4 (over x, core).
Axes of the slice: x: 2, y: 2, z: 4, core: 2. Of those that a mesh axis runs over, the one named last changes fastest.
Arguments:
- spectrum: float32 [1152, 32, 4096], P('comp', 'band'), may hold values from 0.1 to 1
- currents: float32 [2, 32, 4096], P(None, 'band', 'comp'), may hold values from -4 to 4
- group_courant: float32 [32], replicated, may hold values from 0.1 to 0.35
- refraction: float32 [8, 32], replicated, may hold values from -0.25 to 0.25
- interp: float32 [1152, 1152], replicated, may hold values from -0.1875 to 0.1875
- sea_mask: int32 [32, 4096], replicated, may hold values 0 or 1
- depth_class: int32 [32, 4096], replicated, may hold values from 0 to 7
- owner_map: int32 [8], replicated, may hold values from 0 to 7, each once
Outputs:
- spectrum_out: float32 [1152, 32, 4096], P('comp', 'band')
- ocean_out: float32 [2, 32, 4096], P(None, 'band', 'comp')
The draws below stay inside these ranges and needn't reach their ends.
Inputs may be any that keep to these rules, and one draw needn't show every extreme that they name: `owner_map`: each of 0 to 7 once.
All inputs are finite; a program needn't handle non-finite values.
Results may differ from the reference program's by a relative error of at most 0.000098.
Values sent between devices are 32-bit elements; how exact they have to be, the bound alone decides.
No kernel may reach another device: no remote copies, remote signals or barrier semaphores. Data moves between devices by JAX's collectives and lax.ppermute only.
A program may use at most 192 MiB of HBM per device.

```python
import math
import jax
import jax.numpy as jnp
from jax import lax

DIRS = 36
FREQ = 32
CLASSES = 8
SUBSTEPS = 4
LON = 4096
COMPS = 1152
ROWS = 32
TILES = 8


def place_ends(values, own_key, least, largest):
    dims = values.shape
    place = [jax.random.randint(jax.random.fold_in(own_key, axis), (), 0, dims[axis]) for axis in range(len(dims))]
    values = values.at[tuple(place)].set(least)
    longest = dims.index(max(dims))
    place[longest] = (place[longest] + 1) % dims[longest]
    return values.at[tuple(place)].set(largest)


def shard_levels(key, dims, cuts, low, largest):
    def one(position, shards_of):
        heights = jax.random.uniform(jax.random.fold_in(jax.random.fold_in(key, 6), position), (shards_of,), jnp.float32, low / len(cuts), largest / len(cuts))
        return jnp.repeat(jnp.exp(heights), dims[position] // shards_of).reshape((-1,) + (1,) * (len(dims) - position - 1))

    level = one(*cuts[0])
    for cut in cuts[1:]:
        level = level * one(*cut)
    return level


def scatter_about(stream_key, shape, spread, most, shards=(), held_as=jnp.bfloat16):
    array = spread * jax.random.normal(stream_key, shape, jnp.float32)
    if shards:
        array = array * shard_levels(stream_key, shape, shards, -0.22, 0.18)
    return jnp.clip(array, -most, most).astype(held_as)


def setup_inputs(seed: int = 0) -> dict:
    splits = jax.random.split(jax.random.key(seed), 9)
    return {
        "spectrum": jnp.clip(jnp.exp(math.log(1.0) - 2.3025851 * jax.random.uniform(splits[0], (COMPS, ROWS, LON), jnp.float32) ** shard_levels(splits[0], (COMPS, ROWS, LON), ((0, 8), (1, 4)), -0.2, 0.2)), 0.1, 1.0),
        "currents": scatter_about(splits[1], (2, ROWS, LON), 1.0, 4.0, ((1, 4), (2, 8)), jnp.float32),
        "group_courant": jnp.clip(jnp.exp(jax.random.uniform(splits[2], (FREQ,), jnp.float32, math.log(0.1), math.log(0.35))), 0.1, 0.35),
        "refraction": jnp.clip(jax.random.uniform(splits[3], (CLASSES, FREQ), jnp.float32, -0.25, 0.25), -0.25, 0.25),
        "interp": scatter_about(splits[4], (COMPS, COMPS), COMPS ** -0.5, 0.1875, (), jnp.float32),
        "sea_mask": place_ends((jax.random.randint(splits[5], (ROWS, LON), 0, 4) < 3).astype(jnp.int32), jax.random.fold_in(splits[5], 1), 0, 1),
        "depth_class": place_ends(jax.random.randint(splits[6], (ROWS, LON), 0, CLASSES), jax.random.fold_in(splits[6], 1), 0, CLASSES - 1).astype(jnp.int32),
        "owner_map": jax.random.permutation(splits[7], TILES).astype(jnp.int32),
    }


CURRENT_COURANT = 0.025
SOURCE_STEP = 0.5
STOKES_SCALE = 0.2
OCEAN_STEP = 0.5
VISCOSITY = 0.2
DRAG = 0.1
HIGHEST = lax.Precision.HIGHEST


def reorder_tiles(values_in, tile_order, tile_count):
    lead_dim, row_count, col_count = values_in.shape
    pieces = values_in.reshape(lead_dim, row_count, tile_count, col_count // tile_count)
    return jnp.take(pieces, tile_order, axis=2).reshape(lead_dim, row_count, col_count)


def upwind(centre_val, behind, ahead_val, speeds):
    return jnp.maximum(speeds, 0.0) * (centre_val - behind) + jnp.minimum(speeds, 0.0) * (ahead_val - centre_val)


def stokes_weights():
    component = jnp.arange(COMPS, dtype=jnp.int32)
    frequency = component // DIRS
    direction = component % DIRS
    angles = direction.astype(jnp.float32) * (2.0 * math.pi / DIRS)
    scales = STOKES_SCALE * (frequency + 1).astype(jnp.float32) / FREQ
    return jnp.stack([scales * jnp.cos(angles), scales * jnp.sin(angles)])


def reference(spectrum, currents, group_courant, refraction, interp, sea_mask, depth_class, owner_map):
    ocean_field = sea_mask.astype(jnp.float32)
    inverse = jnp.argsort(owner_map).astype(jnp.int32)
    current_real = reorder_tiles(currents, inverse, TILES)
    direction = jnp.arange(DIRS, dtype=jnp.int32)
    angles = direction.astype(jnp.float32) * (2.0 * math.pi / DIRS)
    cosine = jnp.cos(angles)[:, None, None]
    sines = jnp.sin(angles)[:, None, None]
    lon_base = CURRENT_COURANT * current_real[0]
    lat_base = CURRENT_COURANT * current_real[1]

    def one_frequency(inputs):
        wave_block, speeds, table = inputs
        lon_speed = speeds * cosine + lon_base[None]
        lat_speed = speeds * sines + lat_base[None]
        turning = jnp.take(table, depth_class)
        dir_speed = turning[None] * cosine
        for substep in range(SUBSTEPS):
            padded = jnp.pad(wave_block, ((0, 0), (1, 1), (0, 0)))
            centre = padded[:, 1:-1]
            south_rows = padded[:, :-2]
            north_rows = padded[:, 2:]
            west_cols = jnp.roll(centre, 1, axis=2)
            east_cols = jnp.roll(centre, -1, axis=2)
            before_dir = jnp.roll(centre, 1, axis=0)
            after_dir = jnp.roll(centre, -1, axis=0)
            change = upwind(centre, west_cols, east_cols, lon_speed) + upwind(centre, south_rows, north_rows, lat_speed) + upwind(centre, before_dir, after_dir, dir_speed)
            wave_block = ocean_field[None] * (centre - change)
        return wave_block

    blocks = (spectrum * ocean_field[None]).reshape(FREQ, DIRS, ROWS, LON)
    wave_state = lax.map(one_frequency, (blocks, group_courant, jnp.transpose(refraction)))
    flat_state = wave_state.reshape(COMPS, ROWS, LON)
    weights = stokes_weights()

    def one_row(row_index):
        wave_row = lax.dynamic_index_in_dim(flat_state, row_index, 1, keepdims=False)
        forward = jnp.dot(interp, wave_row, precision=HIGHEST, preferred_element_type=jnp.float32)
        backward = jnp.dot(jnp.transpose(interp), wave_row, precision=HIGHEST, preferred_element_type=jnp.float32)
        updated = wave_row + SOURCE_STEP * (forward * backward - 0.5 * wave_row * (forward + backward))
        drift_row = jnp.dot(weights, updated, precision=HIGHEST, preferred_element_type=jnp.float32)
        return updated, drift_row

    updated_rows, drift_rows = lax.map(one_row, jnp.arange(ROWS, dtype=jnp.int32))
    spectrum_out = jnp.moveaxis(updated_rows, 0, 1)
    stokes = jnp.moveaxis(drift_rows, 0, 1)

    masked_cur = current_real * ocean_field[None]
    padded_cur = jnp.pad(masked_cur, ((0, 0), (1, 1), (0, 0)))
    laplace = jnp.roll(masked_cur, 1, axis=2) + jnp.roll(masked_cur, -1, axis=2) + padded_cur[:, :-2] + padded_cur[:, 2:] - 4.0 * masked_cur
    latitude = -1.2 + 2.4 * (jnp.arange(ROWS, dtype=jnp.int32).astype(jnp.float32) + 0.5) / ROWS
    coriolis = jnp.sin(latitude)[:, None]
    east_new = ocean_field * (masked_cur[0] + OCEAN_STEP * (coriolis * (masked_cur[1] + stokes[1]) + VISCOSITY * laplace[0] - DRAG * masked_cur[0]))
    north_new = ocean_field * (masked_cur[1] + OCEAN_STEP * (-coriolis * (masked_cur[0] + stokes[0]) + VISCOSITY * laplace[1] - DRAG * masked_cur[1]))
    ocean_out = reorder_tiles(jnp.stack([east_new, north_new]), owner_map, TILES)
    return spectrum_out, ocean_out
```

```python
import functools
import math

import jax
import jax.numpy as jnp
from jax import lax
from jax.experimental import pallas as pl
from jax.experimental.pallas import tpu as pltpu
from jax.sharding import PartitionSpec as P


DIRS = 36
FREQ = 32
SUBSTEPS = 4


CURRENT_COURANT = 0.025
SOURCE_STEP = 0.5
STOKES_SCALE = 0.2
OCEAN_STEP = 0.5
VISCOSITY = 0.2
DRAG = 0.1
HIGHEST = lax.Precision.HIGHEST


def swapped(block, axis, apart):
    count = lax.axis_size(axis)
    route = []
    for low in range(count):
        high = low | 1 << apart
        if high != low and high < count:
            route += [(low, high), (high, low)]
    return lax.ppermute(block, axis, route)


def padded_2(value, sides, width):
    for axis, dim in sides:
        count, length = (lax.axis_size(axis), value.shape[dim])
        up = [(i, (i + 1) % count) for i in range(count - 1)]
        down = [(j, i) for i, j in up]
        last = lax.slice_in_dim(value, length - width, length, axis=dim)
        first = lax.slice_in_dim(value, 0, width, axis=dim)
        before = lax.ppermute(last, axis, up)
        after = lax.ppermute(first, axis, down)
        value = jnp.concatenate([before, value, after], axis=dim)
    return value


def reorder_tiles(values_in, tile_order, tile_count):
    lead_dim, row_count, col_count = values_in.shape
    pieces = values_in.reshape(lead_dim, row_count, tile_count, col_count // tile_count)
    return jnp.take(pieces, tile_order, axis=2).reshape(lead_dim, row_count, col_count)


def upwind(centre_val, behind, ahead_val, speeds):
    return jnp.maximum(speeds, 0.0) * (centre_val - behind) + jnp.minimum(speeds, 0.0) * (
        ahead_val - centre_val
    )


def direction_pair(centre):
    dir_count, row_count, col_count = centre.shape
    if dir_count % DIRS == 0:
        circles = centre.reshape(dir_count // DIRS, DIRS, row_count, col_count)
        before_dir = jnp.roll(circles, 1, axis=1).reshape(centre.shape)
        after_dir = jnp.roll(circles, -1, axis=1).reshape(centre.shape)
    else:
        edge_dirs = jnp.stack([centre[0], centre[dir_count - 1]])
        partner = swapped(edge_dirs, "comp", 0)
        before_dir = jnp.concatenate([partner[1:2], centre[: dir_count - 1]], axis=0)
        after_dir = jnp.concatenate([centre[1:], partner[0:1]], axis=0)
    return (before_dir, after_dir)


def advance(padded, lon_speed, lat_speed, dir_speed, ocean_rows):
    centre = padded[:, 1:-1]
    south_rows = padded[:, :-2]
    north_rows = padded[:, 2:]
    west_cols = jnp.roll(centre, 1, axis=2)
    east_cols = jnp.roll(centre, -1, axis=2)
    before_dir, after_dir = direction_pair(centre)
    change = (
        upwind(centre, west_cols, east_cols, lon_speed)
        + upwind(centre, south_rows, north_rows, lat_speed)
        + upwind(centre, before_dir, after_dir, dir_speed)
    )
    return ocean_rows[None] * (centre - change)


def coefficients(current_rows, class_rows, speeds, cosine, sines, columns):
    lon_speed = (
        speeds[:, None, None] * cosine[:, None, None] + CURRENT_COURANT * current_rows[0][None]
    )
    lat_speed = (
        speeds[:, None, None] * sines[:, None, None] + CURRENT_COURANT * current_rows[1][None]
    )
    turning = jnp.zeros((speeds.shape[0],) + class_rows.shape, jnp.float32)
    for level in range(columns.shape[0]):
        turning = (
            turning
            + (class_rows == level).astype(jnp.float32)[None] * columns[level][:, None, None]
        )
    return (lon_speed, lat_speed, turning * cosine[:, None, None])


def component_tables(component, group_courant, refraction):
    frequency = component // DIRS
    direction = component % DIRS
    angles = direction.astype(jnp.float32) * (2.0 * math.pi / DIRS)
    return (
        jnp.take(group_courant, frequency),
        jnp.cos(angles),
        jnp.sin(angles),
        jnp.take(refraction, frequency, axis=1),
    )


def stokes_weights(comp_total):
    component = jnp.arange(comp_total, dtype=jnp.int32)
    frequency = component // DIRS
    direction = component % DIRS
    angles = direction.astype(jnp.float32) * (2.0 * math.pi / DIRS)
    scales = STOKES_SCALE * (frequency + 1).astype(jnp.float32) / FREQ
    return jnp.stack([scales * jnp.cos(angles), scales * jnp.sin(angles)])


def source_local(points, interp, weights):
    comp_total, row_count, col_count = points.shape
    flat_spec = points.reshape(comp_total, row_count * col_count)
    forward = jnp.dot(interp, flat_spec, precision=HIGHEST, preferred_element_type=jnp.float32)
    backward = lax.dot_general(
        interp,
        flat_spec,
        (((0,), (0,)), ((), ())),
        precision=HIGHEST,
        preferred_element_type=jnp.float32,
    )
    updated = flat_spec + SOURCE_STEP * (
        forward * backward - 0.5 * flat_spec * (forward + backward)
    )
    drift_rows = jnp.dot(weights, updated, precision=HIGHEST, preferred_element_type=jnp.float32)
    return (
        updated.reshape(comp_total, row_count, col_count),
        drift_rows.reshape(2, row_count, col_count),
    )


def velocity_rows(current_real):
    return padded_2(current_real, (("band", 1),), 1)


def ocean_update(current_rows, ocean_rows, tile_index, tile_width, stokes, coriolis):
    wrapped = jnp.concatenate(
        [current_rows[:, :, -1:], current_rows, current_rows[:, :, :1]], axis=2
    )
    ocean_wrapped = jnp.concatenate([ocean_rows[:, -1:], ocean_rows, ocean_rows[:, :1]], axis=1)
    tile_start = tile_index * tile_width
    cur_tile = lax.dynamic_slice_in_dim(wrapped, tile_start, tile_width + 2, 2)
    ocean_tile = lax.dynamic_slice_in_dim(ocean_wrapped, tile_start, tile_width + 2, 1)
    masked_cur = cur_tile * ocean_tile[None]
    centre = masked_cur[:, 1:-1, 1:-1]
    laplace = (
        masked_cur[:, 1:-1, :-2]
        + masked_cur[:, 1:-1, 2:]
        + masked_cur[:, :-2, 1:-1]
        + masked_cur[:, 2:, 1:-1]
        - 4.0 * centre
    )
    sea_tile = ocean_tile[1:-1, 1:-1]
    east_new = sea_tile * (
        centre[0]
        + OCEAN_STEP
        * (coriolis * (centre[1] + stokes[1]) + VISCOSITY * laplace[0] - DRAG * centre[0])
    )
    north_new = sea_tile * (
        centre[1]
        + OCEAN_STEP
        * (-coriolis * (centre[0] + stokes[0]) + VISCOSITY * laplace[1] - DRAG * centre[1])
    )
    return jnp.stack([east_new, north_new])


def local(spectrum, currents, group_courant, refraction, interp, sea_mask, depth_class, owner_map):
    per_device, rows_dev, lon_cells = spectrum.shape
    tile_count = lax.axis_size("comp")
    tile_width = lon_cells // tile_count
    band_pos = lax.axis_index("band")
    comp_pos = lax.axis_index("comp")
    inverse = jnp.argsort(owner_map)
    gathered = lax.all_gather(currents, "comp", axis=2, tiled=True)
    current_real = reorder_tiles(gathered, inverse, tile_count)
    ocean_pad = jnp.pad(sea_mask.astype(jnp.float32), ((SUBSTEPS, SUBSTEPS), (0, 0)))
    class_pad = jnp.pad(depth_class, ((SUBSTEPS, SUBSTEPS), (0, 0)))
    own_start = band_pos * rows_dev + SUBSTEPS
    ocean_own = lax.dynamic_slice_in_dim(ocean_pad, own_start, rows_dev, 0)
    class_own = lax.dynamic_slice_in_dim(class_pad, own_start, rows_dev, 0)
    weights = stokes_weights(interp.shape[0])
    component = comp_pos * per_device + jnp.arange(per_device, dtype=jnp.int32)
    speeds, cosine, sines, columns = component_tables(component, group_courant, refraction)
    wave_state = spectrum * ocean_own[None]
    lon_speed, lat_speed, dir_speed = coefficients(
        current_real, class_own, speeds, cosine, sines, columns
    )
    for _ in range(SUBSTEPS):
        padded = padded_2(wave_state, (("band", 1),), 1)
        wave_state = advance(padded, lon_speed, lat_speed, dir_speed, ocean_own)
    current_rows = velocity_rows(current_real)
    block_len = rows_dev * lon_cells // tile_count
    blocked = wave_state.reshape(per_device, tile_count, block_len)
    points = lax.all_to_all(blocked, "comp", split_axis=1, concat_axis=0, tiled=True)
    updated, drift_block = source_local(points, interp, weights)
    returned = lax.all_to_all(updated, "comp", split_axis=0, concat_axis=1, tiled=True)
    spectrum_out = returned.reshape(per_device, rows_dev, lon_cells)
    drift_all = lax.all_gather(drift_block, "comp", axis=1, tiled=True).reshape(
        2, rows_dev, lon_cells
    )
    stokes = lax.dynamic_slice_in_dim(drift_all, owner_map[comp_pos] * tile_width, tile_width, 2)
    ocean_rows = lax.dynamic_slice_in_dim(ocean_pad, own_start - 1, rows_dev + 2, 0)
    total_rows = sea_mask.shape[0]
    row_global = band_pos * rows_dev + jnp.arange(rows_dev, dtype=jnp.int32)
    latitude = -1.2 + 2.4 * (row_global.astype(jnp.float32) + 0.5) / total_rows
    coriolis = jnp.sin(latitude)[:, None]
    tile_index = owner_map[comp_pos]
    ocean_out = ocean_update(current_rows, ocean_rows, tile_index, tile_width, stokes, coriolis)
    return (spectrum_out, ocean_out)


SUBLANES = 8
LANES = 128
HALVES = 2


def partner_routes(count, step):
    return [(i, i ^ step) for i in range(count)]


def wave_kernel(
    order_ref, courant_ref, refract_ref, angle_ref, spec_ref, gathered_ref, north_ref, south_ref, ocean_ref, class_ref,
    *rest, group, groups, pieces, parts
):
    outs = rest[:pieces]
    own_a, halo_a, own_b, halo_b, stage, vel, turn, in_sems, out_sems = rest[pieces:]
    dirs, rows, width = own_a.shape
    tiles = width // LANES
    count = gathered_ref.shape[0]
    tile_width = width // count
    per_tile = tile_width // LANES
    per_part = per_tile // parts
    me = lax.axis_index("comp")
    frequency = me * groups + group
    loads = [pltpu.make_async_copy(spec_ref.at[pl.ds(group * dirs, dirs)], own_a, in_sems.at[0])]
    for j in range(count):
        start = pl.multiple_of(order_ref[me ^ j] * tile_width, LANES)
        loads.append(
            pltpu.make_async_copy(gathered_ref.at[j], vel.at[:, :, pl.ds(start, tile_width)], in_sems.at[1 + j])
        )
    for load in loads:
        load.start()
    turning = jnp.zeros(class_ref.shape, jnp.float32)
    for level in range(refract_ref.shape[0]):
        turning = jnp.where(class_ref[...] == level, refract_ref[level, frequency], turning)
    turn[...] = turning
    for load in loads:
        load.wait()
    vel[...] = vel[...] * CURRENT_COURANT

    def enter(d, carry):
        own_a[d] = own_a[d] * ocean_ref[0:rows, :]
        halo_a[d] = jnp.concatenate([north_ref[d], south_ref[d]], axis=0) * ocean_ref[rows : 2 * rows, :]
        return carry

    lax.fori_loop(0, dirs, enter, 0)
    speed = courant_ref[frequency]
    lane = lax.broadcasted_iota(jnp.int32, (rows, LANES), 1)
    row = lax.broadcasted_iota(jnp.int32, (rows, LANES), 0)
    is_first_lane = lane == 0
    is_last_lane = lane == LANES - 1
    is_first_row = row == 0
    is_last_row = row == rows - 1

    def substep(own, halo, own_next, halo_next, last):
        def one_direction(d, carry):
            before = jnp.where(d == 0, dirs - 1, d - 1)
            after = jnp.where(d == dirs - 1, 0, d + 1)
            cosine = angle_ref[0, d]
            speed_x = speed * cosine
            speed_y = speed * angle_ref[1, d]
            cache = {}

            def tile_of(field, name, at):
                key = (name, at)
                if key not in cache:
                    value = field[d, :, at * LANES : (at + 1) * LANES]
                    cache[key] = (value, pltpu.roll(value, 1, 1), pltpu.roll(value, LANES - 1, 1))
                return cache[key]

            def advanced(field, name, at, south, north, part):
                value, up, down = tile_of(field, name, at)
                west = jnp.where(is_first_lane, tile_of(field, name, (at - 1) % tiles)[1], up)
                east = jnp.where(is_last_lane, tile_of(field, name, (at + 1) % tiles)[2], down)
                cols = slice(at * LANES, (at + 1) * LANES)
                span = slice(part * rows, (part + 1) * rows)
                along = speed_x + vel[0, span, cols]
                across = speed_y + vel[1, span, cols]
                turned = turn[span, cols] * cosine
                ahead = field[after, :, cols]
                behind = field[before, :, cols]
                result = value - jnp.abs(along) * (value - jnp.where(along > 0.0, west, east))
                result = result - jnp.abs(across) * (value - jnp.where(across > 0.0, south, north))
                result = result - jnp.abs(turned) * (value - jnp.where(turned > 0.0, behind, ahead))
                return ocean_ref[span, cols] * result

            for at in range(tiles):
                mine = tile_of(own, "own", at)[0]
                cols = slice(at * LANES, (at + 1) * LANES)
                other = halo[d, :, cols]
                own_up = pltpu.roll(mine, 1, 0)
                own_down = pltpu.roll(mine, rows - 1, 0)
                halo_up = pltpu.roll(other, 1, 0)
                halo_down = pltpu.roll(other, rows - 1, 0)
                south = jnp.where(is_first_row, halo_up, own_up)
                north = jnp.where(is_last_row, halo_down, own_down)
                result = advanced(own, "own", at, south, north, 0)
                if last:
                    stage[at // per_tile, at % per_tile, d] = result
                else:
                    own_next[d, :, cols] = result
                    south = jnp.where(is_first_row, own_up, halo_up)
                    north = jnp.where(is_last_row, own_down, halo_down)
                    halo_next[d, :, cols] = advanced(halo, "halo", at, south, north, 1)
            return carry

        lax.fori_loop(0, dirs, one_direction, 0)

    def two_substeps(turn_count, carry):
        substep(own_a, halo_a, own_b, halo_b, False)

        @pl.when(turn_count < SUBSTEPS // 2 - 1)
        def _():
            substep(own_b, halo_b, own_a, halo_a, False)

        return carry

    lax.fori_loop(0, SUBSTEPS // 2, two_substeps, 0)
    substep(own_b, halo_b, None, None, True)
    stores = []
    for k in range(count):
        tile = order_ref[me ^ k]
        for part in range(parts):
            n = k * parts + part
            stores.append(
                pltpu.make_async_copy(stage.at[tile, pl.ds(part * per_part, per_part)], outs[n], out_sems.at[n])
            )
    for store in stores:
        store.start()
    for store in stores:
        store.wait()


def wave_group(
    owner_map, courant, refraction, angles, spectrum, gathered, north, south, ocean16, class16, group, groups, parts
):
    _, rows, width = spectrum.shape
    count = gathered.shape[0]
    per_tile = width // count // LANES
    pieces = count * parts
    piece = jax.ShapeDtypeStruct((per_tile // parts, DIRS, rows, LANES), jnp.float32)
    smem = pl.BlockSpec(memory_space=pltpu.SMEM)
    hbm = pl.BlockSpec(memory_space=pltpu.HBM)
    vmem = pl.BlockSpec(memory_space=pltpu.VMEM)
    state = pltpu.VMEM((DIRS, rows, width), jnp.float32)
    return pl.pallas_call(
        functools.partial(wave_kernel, group=group, groups=groups, pieces=pieces, parts=parts),
        out_shape=[piece] * pieces,
        in_specs=[smem, smem, smem, smem, hbm, hbm, vmem, vmem, vmem, vmem],
        out_specs=[hbm] * pieces,
        scratch_shapes=[
            state,
            state,
            state,
            state,
            pltpu.VMEM((count, per_tile, DIRS, rows, LANES), jnp.float32),
            pltpu.VMEM((2, 2 * rows, width), jnp.float32),
            pltpu.VMEM((2 * rows, width), jnp.float32),
            pltpu.SemaphoreType.DMA((count + 1,)),
            pltpu.SemaphoreType.DMA((pieces,)),
        ],
        compiler_params=pltpu.CompilerParams(vmem_limit_bytes=48 * 1024 * 1024),
        cost_estimate=pl.CostEstimate(flops=2_000_000_000, bytes_accessed=20_000_000, transcendentals=0),
        name="wave_group",
    )(owner_map, courant, refraction, angles, spectrum, gathered, north, south, ocean16, class16)


def source_kernel(high_ref, low_ref, weight_ref, *rest, groups, count, offsets):
    ins = rest[: count * groups]
    outs = rest[count * groups : count * groups + count]
    drift_ref, state, result, x_high, x_low, forward, backward, in_sems, out_sems = rest[count * groups + count :]
    lane_tiles, comps, rows, _ = state.shape
    per_device = comps // count
    per_group = per_device // groups
    me = lax.axis_index("comp")
    loads = []
    for k in range(count):
        for g in range(groups):
            n = k * groups + g
            start = (me ^ k) * per_device + g * per_group
            loads.append(
                pltpu.make_async_copy(
                    ins[n].at[pl.ds(offsets[n], lane_tiles)], state.at[:, pl.ds(start, per_group)], in_sems.at[n]
                )
            )
    for load in loads:
        load.start()
    for load in loads:
        load.wait()
    for tile in range(lane_tiles):
        flat = state.at[tile].reshape(comps * rows, LANES)
        flat_out = result.at[tile].reshape(comps * rows, LANES)

        def row_pair(pair, carry):
            left = 2 * pair
            for side in range(2):
                part = flat[pl.ds(left + side, comps, stride=rows), :]
                high = part.astype(jnp.bfloat16)
                cols = slice(side * LANES, (side + 1) * LANES)
                x_high[:, cols] = high
                x_low[:, cols] = (part - high.astype(jnp.float32)).astype(jnp.bfloat16)
            for target, begin in ((forward, 0), (backward, comps)):
                span = slice(begin, begin + comps)
                target[...] = (
                    jnp.dot(high_ref[span, :], x_high[...], preferred_element_type=jnp.float32)
                    + jnp.dot(high_ref[span, :], x_low[...], preferred_element_type=jnp.float32)
                    + jnp.dot(low_ref[span, :], x_high[...], preferred_element_type=jnp.float32)
                )
            for side in range(2):
                cols = slice(side * LANES, (side + 1) * LANES)
                part = flat[pl.ds(left + side, comps, stride=rows), :]
                ahead = forward[:, cols]
                back = backward[:, cols]
                updated = part + SOURCE_STEP * (ahead * back - 0.5 * part * (ahead + back))
                flat_out[pl.ds(left + side, comps, stride=rows), :] = updated
                for axis in range(2):
                    drift_ref[axis, tile, pl.ds(left + side, 1), :] = jnp.sum(
                        updated * weight_ref[axis], axis=0, keepdims=True
                    )
            return carry

        lax.fori_loop(0, rows // 2, row_pair, 0)
    stores = []
    for k in range(count):
        start = (me ^ k) * per_device
        stores.append(pltpu.make_async_copy(result.at[:, pl.ds(start, per_device)], outs[k], out_sems.at[k]))
    for store in stores:
        store.start()
    for store in stores:
        store.wait()


def source_block(high, low, weights, pieces, offsets, lane_tiles, groups, count):
    _, per_group, rows, _ = pieces[0].shape
    per_device = groups * per_group
    comps = count * per_device
    hbm = pl.BlockSpec(memory_space=pltpu.HBM)
    vmem = pl.BlockSpec(memory_space=pltpu.VMEM)
    *outs, drift = pl.pallas_call(
        functools.partial(source_kernel, groups=groups, count=count, offsets=offsets),
        out_shape=[jax.ShapeDtypeStruct((lane_tiles, per_device, rows, LANES), jnp.float32)] * count
        + [jax.ShapeDtypeStruct((2, lane_tiles, rows, LANES), jnp.float32)],
        in_specs=[vmem, vmem, vmem] + [hbm] * (count * groups),
        out_specs=[hbm] * count + [vmem],
        scratch_shapes=[
            pltpu.VMEM((lane_tiles, comps, rows, LANES), jnp.float32),
            pltpu.VMEM((lane_tiles, comps, rows, LANES), jnp.float32),
            pltpu.VMEM((comps, 2 * LANES), jnp.bfloat16),
            pltpu.VMEM((comps, 2 * LANES), jnp.bfloat16),
            pltpu.VMEM((comps, 2 * LANES), jnp.float32),
            pltpu.VMEM((comps, 2 * LANES), jnp.float32),
            pltpu.SemaphoreType.DMA((count * groups,)),
            pltpu.SemaphoreType.DMA((count,)),
        ],
        compiler_params=pltpu.CompilerParams(vmem_limit_bytes=56 * 1024 * 1024),
        cost_estimate=pl.CostEstimate(flops=4_000_000_000, bytes_accessed=40_000_000, transcendentals=0),
        name="source_block",
    )(high, low, weights, *pieces)
    return outs, drift


def place_kernel(order_ref, *rest, count, half, seeded):
    ins = rest[:count]
    out_ref, stage, in_sems, out_sems = rest[count + seeded :]
    lane_tiles = ins[0].shape[0]
    me = lax.axis_index("comp")
    tile_width = out_ref.shape[2] // count
    loads = [pltpu.make_async_copy(ins[k], stage.at[k], in_sems.at[k]) for k in range(count)]
    for load in loads:
        load.start()
    stores = []
    for k in range(count):
        loads[k].wait()
        for tile in range(lane_tiles):
            start = order_ref[me ^ k] * tile_width + (half * lane_tiles + tile) * LANES
            stores.append(
                pltpu.make_async_copy(
                    stage.at[k, tile],
                    out_ref.at[:, :, pl.ds(pl.multiple_of(start, LANES), LANES)],
                    out_sems.at[k * lane_tiles + tile],
                )
            )
            stores[-1].start()
    for store in stores:
        store.wait()


def place_half(owner_map, pieces, target, half, width):
    lane_tiles, per_device, rows, _ = pieces[0].shape
    count = len(pieces)
    seeded = int(target is not None)
    hbm = pl.BlockSpec(memory_space=pltpu.HBM)
    return pl.pallas_call(
        functools.partial(place_kernel, count=count, half=half, seeded=seeded),
        out_shape=jax.ShapeDtypeStruct((per_device, rows, width), jnp.float32),
        in_specs=[pl.BlockSpec(memory_space=pltpu.SMEM)] + [hbm] * (count + seeded),
        out_specs=hbm,
        scratch_shapes=[
            pltpu.VMEM((count, lane_tiles, per_device, rows, LANES), jnp.float32),
            pltpu.SemaphoreType.DMA((count,)),
            pltpu.SemaphoreType.DMA((count * lane_tiles,)),
        ],
        input_output_aliases={1 + count: 0} if seeded else {},
        name="place_half",
    )(owner_map, *pieces, *([target] if seeded else []))


def band_rows(value, dim):
    count, length = (lax.axis_size("band"), value.shape[dim])
    up = [(i, i + 1) for i in range(count - 1)]
    down = [(j, i) for i, j in up]
    last = lax.slice_in_dim(value, length - SUBSTEPS, length, axis=dim)
    first = lax.slice_in_dim(value, 0, SUBSTEPS, axis=dim)
    north = lax.ppermute(first, "band", down)
    south = lax.ppermute(last, "band", up)
    return north, south


def local_fused(spectrum, currents, group_courant, refraction, interp, sea_mask, depth_class, owner_map):
    per_device, rows, width = spectrum.shape
    count = lax.axis_size("comp")
    tile_width = width // count
    groups = per_device // DIRS
    band_pos = lax.axis_index("band")
    comp_pos = lax.axis_index("comp")
    north_cur, south_cur = band_rows(currents, 1)
    stacked = jnp.concatenate([currents, north_cur, south_cur], axis=1)
    gathered = stacked[None]
    step = 1
    while step < count:
        gathered = jnp.concatenate([gathered, lax.ppermute(gathered, "comp", partner_routes(count, step))], axis=0)
        step *= 2
    halo = band_rows(spectrum[:DIRS], 1)

    def sixteen(field):
        padded = jnp.pad(field, ((SUBSTEPS, SUBSTEPS), (0, 0)))
        window = lax.dynamic_slice_in_dim(padded, band_pos * rows, rows + 2 * SUBSTEPS, 0)
        return jnp.concatenate(
            [window[SUBSTEPS : SUBSTEPS + rows], window[SUBSTEPS + rows :], window[:SUBSTEPS]], axis=0
        )

    ocean16 = sixteen(sea_mask.astype(jnp.float32))
    class16 = sixteen(depth_class)
    angles = jnp.arange(DIRS, dtype=jnp.int32).astype(jnp.float32) * (2.0 * math.pi / DIRS)
    angles = jnp.stack([jnp.cos(angles), jnp.sin(angles)])
    steps = list(range(1, count))
    received = {}
    waiting = {}

    def send(g, part, k, piece):
        received[k, g, part] = lax.ppermute(piece, "comp", partner_routes(count, k))

    source = spectrum
    for g in range(groups):
        parts = parts_of(g)
        pieces = wave_group(
            owner_map, group_courant, refraction, angles, spectrum, gathered, *halo, ocean16, class16, g, groups, parts
        )
        interp, source, pieces = lax.optimization_barrier((interp, source, pieces))
        if g < groups - 1:
            halo = band_rows(source[(g + 1) * DIRS : (g + 2) * DIRS], 1)
        for part in range(parts):
            received[0, g, part] = pieces[part]
        for k in steps:
            send(g, 0, k, pieces[k * parts])
            for part in range(1, parts):
                waiting[g, part, k] = pieces[k * parts + part]
    waiting, pieces = lax.optimization_barrier((waiting, pieces))
    for (g, part, k), piece in waiting.items():
        send(g, part, k, piece)
    stacked_interp = jnp.concatenate([interp, interp.T], axis=0)
    rounded = lax.reduce_precision(stacked_interp, 8, 7)
    high = rounded.astype(jnp.bfloat16)
    low = (stacked_interp - rounded).astype(jnp.bfloat16)
    weights = jnp.broadcast_to(stokes_weights(interp.shape[0])[:, :, None], (2, interp.shape[0], LANES))
    lane_tiles = tile_width // LANES // HALVES
    spectrum_out = None
    drifts = []
    returned = []
    for half in range(HALVES):
        blocks, offsets = [], []
        for k in range(count):
            for g in range(groups):
                split = (k, g, 1) in received
                blocks.append(received[k, g, half if split else 0])
                offsets.append(0 if split else half * lane_tiles)
        outs, drift = source_block(high, low, weights, blocks, offsets, lane_tiles, groups, count)
        drifts.append(drift)
        returned.append(
            [outs[0]] + [lax.ppermute(outs[k], "comp", partner_routes(count, k)) for k in steps]
        )
    for half in range(HALVES):
        spectrum_out = place_half(owner_map, returned[half], spectrum_out, half, width)
    stokes = jnp.concatenate(drifts, axis=1).transpose(0, 2, 1, 3).reshape(2, rows, tile_width)
    tile_index = owner_map[comp_pos]
    order = owner_map[comp_pos ^ jnp.arange(count, dtype=jnp.int32)]
    last_cols = gathered[:, :, :, -1]
    first_cols = gathered[:, :, :, 0]

    def picked(cols, tile):
        chosen = (order == tile % count)[:, None, None]
        return jnp.sum(jnp.where(chosen, cols, 0.0), axis=0)[:, :, None]

    around = jnp.concatenate(
        [picked(last_cols, tile_index + count - 1), stacked, picked(first_cols, tile_index + 1)], axis=2
    )
    wrapped = jnp.concatenate([ocean16[:, -1:], ocean16, ocean16[:, :1]], axis=1)
    sea = lax.dynamic_slice_in_dim(wrapped, tile_index * tile_width, tile_width + 2, 1)
    masked = around * sea[None]
    extended = jnp.concatenate(
        [masked[:, 2 * rows - 1 :], masked[:, :rows], masked[:, rows : rows + 1]], axis=1
    )
    centre = extended[:, 1:-1, 1:-1]
    laplace = (
        extended[:, 1:-1, :-2]
        + extended[:, 1:-1, 2:]
        + extended[:, :-2, 1:-1]
        + extended[:, 2:, 1:-1]
        - 4.0 * centre
    )
    sea_tile = sea[:rows, 1:-1]
    row_global = band_pos * rows + jnp.arange(rows, dtype=jnp.int32)
    latitude = -1.2 + 2.4 * (row_global.astype(jnp.float32) + 0.5) / sea_mask.shape[0]
    coriolis = jnp.sin(latitude)[:, None]
    east_new = sea_tile * (
        centre[0]
        + OCEAN_STEP * (coriolis * (centre[1] + stokes[1]) + VISCOSITY * laplace[0] - DRAG * centre[0])
    )
    north_new = sea_tile * (
        centre[1]
        + OCEAN_STEP * (-coriolis * (centre[0] + stokes[0]) + VISCOSITY * laplace[1] - DRAG * centre[1])
    )
    return (spectrum_out, jnp.stack([east_new, north_new]))


def parts_of(group):
    return 1 if group == 0 else HALVES


def fits(mesh, spectrum):
    comps, rows_all, width = spectrum.shape
    count = mesh.shape["comp"]
    return (
        (comps // count) % DIRS == 0
        and count & (count - 1) == 0
        and rows_all // mesh.shape["band"] == SUBLANES
        and width % (count * HALVES * LANES) == 0
    )


def solution(mesh):
    in_specs = (P("comp", "band", None), P(None, "band", "comp"), P(), P(), P(), P(), P(), P())
    out_specs = (P("comp", "band", None), P(None, "band", "comp"))
    shard = functools.partial(jax.shard_map, mesh=mesh, in_specs=in_specs, out_specs=out_specs, check_vma=False)

    def step(spectrum, *others):
        if not fits(mesh, spectrum):
            return shard(local)(spectrum, *others)

        return shard(local_fused)(spectrum, *others)

    return step
```

```python
import functools
import math

import jax
import jax.numpy as jnp
from jax import lax
from jax.experimental import pallas as pl
from jax.experimental.pallas import tpu as pltpu
from jax.sharding import PartitionSpec as P


DIRS = 36
FREQ = 32
SUBSTEPS = 4


CURRENT_COURANT = 0.025
SOURCE_STEP = 0.5
STOKES_SCALE = 0.2
OCEAN_STEP = 0.5
VISCOSITY = 0.2
DRAG = 0.1
HIGHEST = lax.Precision.HIGHEST


def swapped(block, axis, apart):
    count = lax.axis_size(axis)
    route = []
    for low in range(count):
        high = low | 1 << apart
        if high != low and high < count:
            route += [(low, high), (high, low)]
    return lax.ppermute(block, axis, route)


def padded_2(value, sides, width):
    for axis, dim in sides:
        count, length = (lax.axis_size(axis), value.shape[dim])
        up = [(i, (i + 1) % count) for i in range(count - 1)]
        down = [(j, i) for i, j in up]
        last = lax.slice_in_dim(value, length - width, length, axis=dim)
        first = lax.slice_in_dim(value, 0, width, axis=dim)
        before = lax.ppermute(last, axis, up)
        after = lax.ppermute(first, axis, down)
        value = jnp.concatenate([before, value, after], axis=dim)
    return value


def reorder_tiles(values_in, tile_order, tile_count):
    lead_dim, row_count, col_count = values_in.shape
    pieces = values_in.reshape(lead_dim, row_count, tile_count, col_count // tile_count)
    return jnp.take(pieces, tile_order, axis=2).reshape(lead_dim, row_count, col_count)


def upwind(centre_val, behind, ahead_val, speeds):
    return jnp.maximum(speeds, 0.0) * (centre_val - behind) + jnp.minimum(speeds, 0.0) * (
        ahead_val - centre_val
    )


def direction_pair(centre):
    dir_count, row_count, col_count = centre.shape
    if dir_count % DIRS == 0:
        circles = centre.reshape(dir_count // DIRS, DIRS, row_count, col_count)
        before_dir = jnp.roll(circles, 1, axis=1).reshape(centre.shape)
        after_dir = jnp.roll(circles, -1, axis=1).reshape(centre.shape)
    else:
        edge_dirs = jnp.stack([centre[0], centre[dir_count - 1]])
        partner = swapped(edge_dirs, "comp", 0)
        before_dir = jnp.concatenate([partner[1:2], centre[: dir_count - 1]], axis=0)
        after_dir = jnp.concatenate([centre[1:], partner[0:1]], axis=0)
    return (before_dir, after_dir)


def advance(padded, lon_speed, lat_speed, dir_speed, ocean_rows):
    centre = padded[:, 1:-1]
    south_rows = padded[:, :-2]
    north_rows = padded[:, 2:]
    west_cols = jnp.roll(centre, 1, axis=2)
    east_cols = jnp.roll(centre, -1, axis=2)
    before_dir, after_dir = direction_pair(centre)
    change = (
        upwind(centre, west_cols, east_cols, lon_speed)
        + upwind(centre, south_rows, north_rows, lat_speed)
        + upwind(centre, before_dir, after_dir, dir_speed)
    )
    return ocean_rows[None] * (centre - change)


def coefficients(current_rows, class_rows, speeds, cosine, sines, columns):
    lon_speed = (
        speeds[:, None, None] * cosine[:, None, None] + CURRENT_COURANT * current_rows[0][None]
    )
    lat_speed = (
        speeds[:, None, None] * sines[:, None, None] + CURRENT_COURANT * current_rows[1][None]
    )
    turning = jnp.zeros((speeds.shape[0],) + class_rows.shape, jnp.float32)
    for level in range(columns.shape[0]):
        turning = (
            turning
            + (class_rows == level).astype(jnp.float32)[None] * columns[level][:, None, None]
        )
    return (lon_speed, lat_speed, turning * cosine[:, None, None])


def component_tables(component, group_courant, refraction):
    frequency = component // DIRS
    direction = component % DIRS
    angles = direction.astype(jnp.float32) * (2.0 * math.pi / DIRS)
    return (
        jnp.take(group_courant, frequency),
        jnp.cos(angles),
        jnp.sin(angles),
        jnp.take(refraction, frequency, axis=1),
    )


def stokes_weights(comp_total):
    component = jnp.arange(comp_total, dtype=jnp.int32)
    frequency = component // DIRS
    direction = component % DIRS
    angles = direction.astype(jnp.float32) * (2.0 * math.pi / DIRS)
    scales = STOKES_SCALE * (frequency + 1).astype(jnp.float32) / FREQ
    return jnp.stack([scales * jnp.cos(angles), scales * jnp.sin(angles)])


def source_local(points, interp, weights):
    comp_total, row_count, col_count = points.shape
    flat_spec = points.reshape(comp_total, row_count * col_count)
    forward = jnp.dot(interp, flat_spec, precision=HIGHEST, preferred_element_type=jnp.float32)
    backward = lax.dot_general(
        interp,
        flat_spec,
        (((0,), (0,)), ((), ())),
        precision=HIGHEST,
        preferred_element_type=jnp.float32,
    )
    updated = flat_spec + SOURCE_STEP * (
        forward * backward - 0.5 * flat_spec * (forward + backward)
    )
    drift_rows = jnp.dot(weights, updated, precision=HIGHEST, preferred_element_type=jnp.float32)
    return (
        updated.reshape(comp_total, row_count, col_count),
        drift_rows.reshape(2, row_count, col_count),
    )


def velocity_rows(current_real):
    return padded_2(current_real, (("band", 1),), 1)


def ocean_update(current_rows, ocean_rows, tile_index, tile_width, stokes, coriolis):
    wrapped = jnp.concatenate(
        [current_rows[:, :, -1:], current_rows, current_rows[:, :, :1]], axis=2
    )
    ocean_wrapped = jnp.concatenate([ocean_rows[:, -1:], ocean_rows, ocean_rows[:, :1]], axis=1)
    tile_start = tile_index * tile_width
    cur_tile = lax.dynamic_slice_in_dim(wrapped, tile_start, tile_width + 2, 2)
    ocean_tile = lax.dynamic_slice_in_dim(ocean_wrapped, tile_start, tile_width + 2, 1)
    masked_cur = cur_tile * ocean_tile[None]
    centre = masked_cur[:, 1:-1, 1:-1]
    laplace = (
        masked_cur[:, 1:-1, :-2]
        + masked_cur[:, 1:-1, 2:]
        + masked_cur[:, :-2, 1:-1]
        + masked_cur[:, 2:, 1:-1]
        - 4.0 * centre
    )
    sea_tile = ocean_tile[1:-1, 1:-1]
    east_new = sea_tile * (
        centre[0]
        + OCEAN_STEP
        * (coriolis * (centre[1] + stokes[1]) + VISCOSITY * laplace[0] - DRAG * centre[0])
    )
    north_new = sea_tile * (
        centre[1]
        + OCEAN_STEP
        * (-coriolis * (centre[0] + stokes[0]) + VISCOSITY * laplace[1] - DRAG * centre[1])
    )
    return jnp.stack([east_new, north_new])


def local(spectrum, currents, group_courant, refraction, interp, sea_mask, depth_class, owner_map):
    per_device, rows_dev, lon_cells = spectrum.shape
    tile_count = lax.axis_size("comp")
    tile_width = lon_cells // tile_count
    band_pos = lax.axis_index("band")
    comp_pos = lax.axis_index("comp")
    inverse = jnp.argsort(owner_map)
    gathered = lax.all_gather(currents, "comp", axis=2, tiled=True)
    current_real = reorder_tiles(gathered, inverse, tile_count)
    ocean_pad = jnp.pad(sea_mask.astype(jnp.float32), ((SUBSTEPS, SUBSTEPS), (0, 0)))
    class_pad = jnp.pad(depth_class, ((SUBSTEPS, SUBSTEPS), (0, 0)))
    own_start = band_pos * rows_dev + SUBSTEPS
    ocean_own = lax.dynamic_slice_in_dim(ocean_pad, own_start, rows_dev, 0)
    class_own = lax.dynamic_slice_in_dim(class_pad, own_start, rows_dev, 0)
    weights = stokes_weights(interp.shape[0])
    component = comp_pos * per_device + jnp.arange(per_device, dtype=jnp.int32)
    speeds, cosine, sines, columns = component_tables(component, group_courant, refraction)
    wave_state = spectrum * ocean_own[None]
    lon_speed, lat_speed, dir_speed = coefficients(
        current_real, class_own, speeds, cosine, sines, columns
    )
    for _ in range(SUBSTEPS):
        padded = padded_2(wave_state, (("band", 1),), 1)
        wave_state = advance(padded, lon_speed, lat_speed, dir_speed, ocean_own)
    current_rows = velocity_rows(current_real)
    block_len = rows_dev * lon_cells // tile_count
    blocked = wave_state.reshape(per_device, tile_count, block_len)
    points = lax.all_to_all(blocked, "comp", split_axis=1, concat_axis=0, tiled=True)
    updated, drift_block = source_local(points, interp, weights)
    returned = lax.all_to_all(updated, "comp", split_axis=0, concat_axis=1, tiled=True)
    spectrum_out = returned.reshape(per_device, rows_dev, lon_cells)
    drift_all = lax.all_gather(drift_block, "comp", axis=1, tiled=True).reshape(
        2, rows_dev, lon_cells
    )
    stokes = lax.dynamic_slice_in_dim(drift_all, owner_map[comp_pos] * tile_width, tile_width, 2)
    ocean_rows = lax.dynamic_slice_in_dim(ocean_pad, own_start - 1, rows_dev + 2, 0)
    total_rows = sea_mask.shape[0]
    row_global = band_pos * rows_dev + jnp.arange(rows_dev, dtype=jnp.int32)
    latitude = -1.2 + 2.4 * (row_global.astype(jnp.float32) + 0.5) / total_rows
    coriolis = jnp.sin(latitude)[:, None]
    tile_index = owner_map[comp_pos]
    ocean_out = ocean_update(current_rows, ocean_rows, tile_index, tile_width, stokes, coriolis)
    return (spectrum_out, ocean_out)


SUBLANES = 8
LANES = 128
BLOCKS = 4


def partner_routes(count, step):
    return [(i, i ^ step) for i in range(count)]


def wave_kernel(
    order_ref, courant_ref, refract_ref, angle_ref, spec_ref, gathered_ref, north_ref, south_ref, ocean_ref, class_ref,
    *rest, group, groups, pieces, parts
):
    outs = rest[:pieces]
    own_a, halo_a, own_b, halo_b, stage, vel, turn, in_sems, out_sems = rest[pieces:]
    dirs, rows, width = own_a.shape
    tiles = width // LANES
    count = gathered_ref.shape[0]
    tile_width = width // count
    per_tile = tile_width // LANES
    begins = [sum(parts[:n]) for n in range(len(parts))]
    me = lax.axis_index("comp")
    frequency = me * groups + group
    loads = [pltpu.make_async_copy(spec_ref.at[pl.ds(group * dirs, dirs)], own_a, in_sems.at[0])]
    for j in range(count):
        start = pl.multiple_of(order_ref[me ^ j] * tile_width, LANES)
        loads.append(
            pltpu.make_async_copy(gathered_ref.at[j], vel.at[:, :, pl.ds(start, tile_width)], in_sems.at[1 + j])
        )
    for load in loads:
        load.start()
    turning = jnp.zeros(class_ref.shape, jnp.float32)
    for level in range(refract_ref.shape[0]):
        turning = jnp.where(class_ref[...] == level, refract_ref[level, frequency], turning)
    turn[...] = turning
    for load in loads:
        load.wait()
    vel[...] = vel[...] * CURRENT_COURANT

    def enter(d, carry):
        own_a[d] = own_a[d] * ocean_ref[0:rows, :]
        halo_a[d] = jnp.concatenate([north_ref[d], south_ref[d]], axis=0) * ocean_ref[rows : 2 * rows, :]
        return carry

    lax.fori_loop(0, dirs, enter, 0)
    speed = courant_ref[frequency]
    lane = lax.broadcasted_iota(jnp.int32, (rows, LANES), 1)
    row = lax.broadcasted_iota(jnp.int32, (rows, LANES), 0)
    is_first_lane = lane == 0
    is_last_lane = lane == LANES - 1
    is_first_row = row == 0
    is_last_row = row == rows - 1

    def substep(own, halo, own_next, halo_next, last):
        def one_direction(d, carry):
            before = jnp.where(d == 0, dirs - 1, d - 1)
            after = jnp.where(d == dirs - 1, 0, d + 1)
            cosine = angle_ref[0, d]
            speed_x = speed * cosine
            speed_y = speed * angle_ref[1, d]
            cache = {}

            def tile_of(field, name, at):
                key = (name, at)
                if key not in cache:
                    value = field[d, :, at * LANES : (at + 1) * LANES]
                    cache[key] = (value, pltpu.roll(value, 1, 1), pltpu.roll(value, LANES - 1, 1))
                return cache[key]

            def advanced(field, name, at, south, north, part):
                value, up, down = tile_of(field, name, at)
                west = jnp.where(is_first_lane, tile_of(field, name, (at - 1) % tiles)[1], up)
                east = jnp.where(is_last_lane, tile_of(field, name, (at + 1) % tiles)[2], down)
                cols = slice(at * LANES, (at + 1) * LANES)
                span = slice(part * rows, (part + 1) * rows)
                along = speed_x + vel[0, span, cols]
                across = speed_y + vel[1, span, cols]
                turned = turn[span, cols] * cosine
                ahead = field[after, :, cols]
                behind = field[before, :, cols]
                result = value - jnp.abs(along) * (value - jnp.where(along > 0.0, west, east))
                result = result - jnp.abs(across) * (value - jnp.where(across > 0.0, south, north))
                result = result - jnp.abs(turned) * (value - jnp.where(turned > 0.0, behind, ahead))
                return ocean_ref[span, cols] * result

            for at in range(tiles):
                mine = tile_of(own, "own", at)[0]
                cols = slice(at * LANES, (at + 1) * LANES)
                other = halo[d, :, cols]
                own_up = pltpu.roll(mine, 1, 0)
                own_down = pltpu.roll(mine, rows - 1, 0)
                halo_up = pltpu.roll(other, 1, 0)
                halo_down = pltpu.roll(other, rows - 1, 0)
                south = jnp.where(is_first_row, halo_up, own_up)
                north = jnp.where(is_last_row, halo_down, own_down)
                result = advanced(own, "own", at, south, north, 0)
                if last:
                    stage[at // per_tile, at % per_tile, d] = result
                else:
                    own_next[d, :, cols] = result
                    south = jnp.where(is_first_row, own_up, halo_up)
                    north = jnp.where(is_last_row, own_down, halo_down)
                    halo_next[d, :, cols] = advanced(halo, "halo", at, south, north, 1)
            return carry

        lax.fori_loop(0, dirs, one_direction, 0)

    def two_substeps(turn_count, carry):
        substep(own_a, halo_a, own_b, halo_b, False)

        @pl.when(turn_count < SUBSTEPS // 2 - 1)
        def _():
            substep(own_b, halo_b, own_a, halo_a, False)

        return carry

    lax.fori_loop(0, SUBSTEPS // 2, two_substeps, 0)
    substep(own_b, halo_b, None, None, True)
    stores = []
    for k in range(count):
        tile = order_ref[me ^ k]
        for part, size in enumerate(parts):
            n = k * len(parts) + part
            stores.append(
                pltpu.make_async_copy(stage.at[tile, pl.ds(begins[part], size)], outs[n], out_sems.at[n])
            )
    for store in stores:
        store.start()
    for store in stores:
        store.wait()


def wave_group(
    owner_map, courant, refraction, angles, spectrum, gathered, north, south, ocean16, class16, group, groups, parts
):
    _, rows, width = spectrum.shape
    count = gathered.shape[0]
    per_tile = width // count // LANES
    pieces = count * len(parts)
    shapes = [jax.ShapeDtypeStruct((size, DIRS, rows, LANES), jnp.float32) for size in parts] * count
    smem = pl.BlockSpec(memory_space=pltpu.SMEM)
    hbm = pl.BlockSpec(memory_space=pltpu.HBM)
    vmem = pl.BlockSpec(memory_space=pltpu.VMEM)
    state = pltpu.VMEM((DIRS, rows, width), jnp.float32)
    return pl.pallas_call(
        functools.partial(wave_kernel, group=group, groups=groups, pieces=pieces, parts=parts),
        out_shape=shapes,
        in_specs=[smem, smem, smem, smem, hbm, hbm, vmem, vmem, vmem, vmem],
        out_specs=[hbm] * pieces,
        scratch_shapes=[
            state,
            state,
            state,
            state,
            pltpu.VMEM((count, per_tile, DIRS, rows, LANES), jnp.float32),
            pltpu.VMEM((2, 2 * rows, width), jnp.float32),
            pltpu.VMEM((2 * rows, width), jnp.float32),
            pltpu.SemaphoreType.DMA((count + 1,)),
            pltpu.SemaphoreType.DMA((pieces,)),
        ],
        compiler_params=pltpu.CompilerParams(vmem_limit_bytes=48 * 1024 * 1024),
        cost_estimate=pl.CostEstimate(flops=2_000_000_000, bytes_accessed=20_000_000, transcendentals=0),
        name="wave_group",
    )(owner_map, courant, refraction, angles, spectrum, gathered, north, south, ocean16, class16)


def source_kernel(high_ref, low_ref, weight_ref, *rest, groups, count, offsets):
    ins = rest[: count * groups]
    outs = rest[count * groups : count * groups + count]
    drift_ref, state, result, x_high, x_low, forward, backward, in_sems, out_sems = rest[count * groups + count :]
    lane_tiles, comps, rows, _ = state.shape
    per_device = comps // count
    per_group = per_device // groups
    me = lax.axis_index("comp")
    loads = []
    for k in range(count):
        for g in range(groups):
            n = k * groups + g
            start = (me ^ k) * per_device + g * per_group
            loads.append(
                pltpu.make_async_copy(
                    ins[n].at[pl.ds(offsets[n], lane_tiles)], state.at[:, pl.ds(start, per_group)], in_sems.at[n]
                )
            )
    for load in loads:
        load.start()
    for load in loads:
        load.wait()
    for tile in range(lane_tiles):
        flat = state.at[tile].reshape(comps * rows, LANES)
        flat_out = result.at[tile].reshape(comps * rows, LANES)

        def row_pair(pair, carry):
            left = 2 * pair
            for side in range(2):
                part = flat[pl.ds(left + side, comps, stride=rows), :]
                high = part.astype(jnp.bfloat16)
                cols = slice(side * LANES, (side + 1) * LANES)
                x_high[:, cols] = high
                x_low[:, cols] = (part - high.astype(jnp.float32)).astype(jnp.bfloat16)
            for target, begin in ((forward, 0), (backward, comps)):
                span = slice(begin, begin + comps)
                target[...] = (
                    jnp.dot(high_ref[span, :], x_high[...], preferred_element_type=jnp.float32)
                    + jnp.dot(high_ref[span, :], x_low[...], preferred_element_type=jnp.float32)
                    + jnp.dot(low_ref[span, :], x_high[...], preferred_element_type=jnp.float32)
                )
            for side in range(2):
                cols = slice(side * LANES, (side + 1) * LANES)
                part = flat[pl.ds(left + side, comps, stride=rows), :]
                ahead = forward[:, cols]
                back = backward[:, cols]
                updated = part + SOURCE_STEP * (ahead * back - 0.5 * part * (ahead + back))
                flat_out[pl.ds(left + side, comps, stride=rows), :] = updated
                for axis in range(2):
                    drift_ref[axis, tile, pl.ds(left + side, 1), :] = jnp.sum(
                        updated * weight_ref[axis], axis=0, keepdims=True
                    )
            return carry

        lax.fori_loop(0, rows // 2, row_pair, 0)
    stores = []
    for k in range(count):
        start = (me ^ k) * per_device
        stores.append(pltpu.make_async_copy(result.at[:, pl.ds(start, per_device)], outs[k], out_sems.at[k]))
    for store in stores:
        store.start()
    for store in stores:
        store.wait()


def source_block(high, low, weights, pieces, offsets, lane_tiles, groups, count):
    _, per_group, rows, _ = pieces[0].shape
    per_device = groups * per_group
    comps = count * per_device
    hbm = pl.BlockSpec(memory_space=pltpu.HBM)
    vmem = pl.BlockSpec(memory_space=pltpu.VMEM)
    *outs, drift = pl.pallas_call(
        functools.partial(source_kernel, groups=groups, count=count, offsets=offsets),
        out_shape=[jax.ShapeDtypeStruct((lane_tiles, per_device, rows, LANES), jnp.float32)] * count
        + [jax.ShapeDtypeStruct((2, lane_tiles, rows, LANES), jnp.float32)],
        in_specs=[vmem, vmem, vmem] + [hbm] * (count * groups),
        out_specs=[hbm] * count + [vmem],
        scratch_shapes=[
            pltpu.VMEM((lane_tiles, comps, rows, LANES), jnp.float32),
            pltpu.VMEM((lane_tiles, comps, rows, LANES), jnp.float32),
            pltpu.VMEM((comps, 2 * LANES), jnp.bfloat16),
            pltpu.VMEM((comps, 2 * LANES), jnp.bfloat16),
            pltpu.VMEM((comps, 2 * LANES), jnp.float32),
            pltpu.VMEM((comps, 2 * LANES), jnp.float32),
            pltpu.SemaphoreType.DMA((count * groups,)),
            pltpu.SemaphoreType.DMA((count,)),
        ],
        compiler_params=pltpu.CompilerParams(vmem_limit_bytes=56 * 1024 * 1024),
        cost_estimate=pl.CostEstimate(flops=4_000_000_000, bytes_accessed=40_000_000, transcendentals=0),
        name="source_block",
    )(high, low, weights, *pieces)
    return outs, drift


def place_kernel(order_ref, *rest, first, count, half, seeded):
    ins = rest[:count]
    out_ref, stage, in_sems, out_sems = rest[count + seeded :]
    lane_tiles = ins[0].shape[0]
    me = lax.axis_index("comp")
    tile_width = out_ref.shape[2] // order_ref.shape[0]
    loads = [pltpu.make_async_copy(ins[k], stage.at[k], in_sems.at[k]) for k in range(count)]
    for load in loads:
        load.start()
    stores = []
    for k in range(count):
        loads[k].wait()
        for tile in range(lane_tiles):
            start = order_ref[me ^ (first + k)] * tile_width + (half * lane_tiles + tile) * LANES
            stores.append(
                pltpu.make_async_copy(
                    stage.at[k, tile],
                    out_ref.at[:, :, pl.ds(pl.multiple_of(start, LANES), LANES)],
                    out_sems.at[k * lane_tiles + tile],
                )
            )
            stores[-1].start()
    for store in stores:
        store.wait()


def place_part(owner_map, pieces, target, half, width, ks):
    lane_tiles, per_device, rows, _ = pieces[0].shape
    pieces = [pieces[k] for k in ks]
    count = len(pieces)
    seeded = int(target is not None)
    hbm = pl.BlockSpec(memory_space=pltpu.HBM)
    return pl.pallas_call(
        functools.partial(place_kernel, first=ks[0], count=count, half=half, seeded=seeded),
        out_shape=jax.ShapeDtypeStruct((per_device, rows, width), jnp.float32),
        in_specs=[pl.BlockSpec(memory_space=pltpu.SMEM)] + [hbm] * (count + seeded),
        out_specs=hbm,
        scratch_shapes=[
            pltpu.VMEM((count, lane_tiles, per_device, rows, LANES), jnp.float32),
            pltpu.SemaphoreType.DMA((count,)),
            pltpu.SemaphoreType.DMA((count * lane_tiles,)),
        ],
        input_output_aliases={1 + count: 0} if seeded else {},
        name="place_part",
    )(owner_map, *pieces, *([target] if seeded else []))


def band_rows(value, dim):
    count, length = (lax.axis_size("band"), value.shape[dim])
    up = [(i, i + 1) for i in range(count - 1)]
    down = [(j, i) for i, j in up]
    last = lax.slice_in_dim(value, length - SUBSTEPS, length, axis=dim)
    first = lax.slice_in_dim(value, 0, SUBSTEPS, axis=dim)
    north = lax.ppermute(first, "band", down)
    south = lax.ppermute(last, "band", up)
    return north, south


def local_fused(spectrum, currents, group_courant, refraction, interp, sea_mask, depth_class, owner_map):
    per_device, rows, width = spectrum.shape
    count = lax.axis_size("comp")
    tile_width = width // count
    groups = per_device // DIRS
    band_pos = lax.axis_index("band")
    comp_pos = lax.axis_index("comp")
    north_cur, south_cur = band_rows(currents, 1)
    stacked = jnp.concatenate([currents, north_cur, south_cur], axis=1)
    gathered = stacked[None]
    step = 1
    while step < count:
        gathered = jnp.concatenate([gathered, lax.ppermute(gathered, "comp", partner_routes(count, step))], axis=0)
        step *= 2
    halo = band_rows(spectrum[:DIRS], 1)

    def sixteen(field):
        padded = jnp.pad(field, ((SUBSTEPS, SUBSTEPS), (0, 0)))
        window = lax.dynamic_slice_in_dim(padded, band_pos * rows, rows + 2 * SUBSTEPS, 0)
        return jnp.concatenate(
            [window[SUBSTEPS : SUBSTEPS + rows], window[SUBSTEPS + rows :], window[:SUBSTEPS]], axis=0
        )

    ocean16 = sixteen(sea_mask.astype(jnp.float32))
    class16 = sixteen(depth_class)
    angles = jnp.arange(DIRS, dtype=jnp.int32).astype(jnp.float32) * (2.0 * math.pi / DIRS)
    angles = jnp.stack([jnp.cos(angles), jnp.sin(angles)])
    steps = list(range(1, count))
    received = {}
    waiting = {}

    def send(g, part, k, piece):
        received[k, g, part] = lax.ppermute(piece, "comp", partner_routes(count, k))

    source = spectrum
    for g in range(groups):
        parts = parts_of(g, groups, tile_width // LANES)
        pieces = wave_group(
            owner_map, group_courant, refraction, angles, spectrum, gathered, *halo, ocean16, class16, g, groups, parts
        )
        interp, source, pieces = lax.optimization_barrier((interp, source, pieces))
        if g == 0:
            stacked_interp = jnp.concatenate([interp, interp.T], axis=0)
            rounded = lax.reduce_precision(stacked_interp, 8, 7)
            high = rounded.astype(jnp.bfloat16)
            low = (stacked_interp - rounded).astype(jnp.bfloat16)
            class16, high, low = lax.optimization_barrier((class16, high, low))
        if g < groups - 1:
            halo = band_rows(source[(g + 1) * DIRS : (g + 2) * DIRS], 1)
        for part in range(len(parts)):
            received[0, g, part] = pieces[part]
        for k in steps:
            send(g, 0, k, pieces[k * len(parts)])
            for part in range(1, len(parts)):
                waiting[g, part, k] = pieces[k * len(parts) + part]
    waiting, received = lax.optimization_barrier((waiting, received))
    for (g, part, k), piece in waiting.items():
        send(g, part, k, piece)
    weights = jnp.broadcast_to(stokes_weights(interp.shape[0])[:, :, None], (2, interp.shape[0], LANES))
    lane_tiles = tile_width // LANES // BLOCKS
    spectrum_out = None
    drifts = []
    returned = []
    for half in range(BLOCKS):
        blocks, offsets = [], []
        for k in range(count):
            for g in range(groups):
                split = (k, g, 1) in received
                part = int(split and half > 0)
                blocks.append(received[k, g, part])
                offsets.append((half - part) * lane_tiles)
        outs, drift = source_block(high, low, weights, blocks, offsets, lane_tiles, groups, count)
        drifts.append(drift)
        back = [outs[0]]
        for k in steps:
            back.append(lax.ppermute(outs[k], "comp", partner_routes(count, k)))
        returned.append(back)
    for half in range(BLOCKS):
        cuts = [0, count] if half < BLOCKS - 1 else [0, count // 2, count]
        for ks in map(range, cuts[:-1], cuts[1:]):
            spectrum_out = place_part(owner_map, returned[half], spectrum_out, half, width, ks)
    stokes = jnp.concatenate(drifts, axis=1).transpose(0, 2, 1, 3).reshape(2, rows, tile_width)
    tile_index = owner_map[comp_pos]
    order = owner_map[comp_pos ^ jnp.arange(count, dtype=jnp.int32)]
    last_cols = gathered[:, :, :, -1]
    first_cols = gathered[:, :, :, 0]

    def picked(cols, tile):
        chosen = (order == tile % count)[:, None, None]
        return jnp.sum(jnp.where(chosen, cols, 0.0), axis=0)[:, :, None]

    around = jnp.concatenate(
        [picked(last_cols, tile_index + count - 1), stacked, picked(first_cols, tile_index + 1)], axis=2
    )
    wrapped = jnp.concatenate([ocean16[:, -1:], ocean16, ocean16[:, :1]], axis=1)
    sea = lax.dynamic_slice_in_dim(wrapped, tile_index * tile_width, tile_width + 2, 1)
    masked = around * sea[None]
    extended = jnp.concatenate(
        [masked[:, 2 * rows - 1 :], masked[:, :rows], masked[:, rows : rows + 1]], axis=1
    )
    centre = extended[:, 1:-1, 1:-1]
    laplace = (
        extended[:, 1:-1, :-2]
        + extended[:, 1:-1, 2:]
        + extended[:, :-2, 1:-1]
        + extended[:, 2:, 1:-1]
        - 4.0 * centre
    )
    sea_tile = sea[:rows, 1:-1]
    row_global = band_pos * rows + jnp.arange(rows, dtype=jnp.int32)
    latitude = -1.2 + 2.4 * (row_global.astype(jnp.float32) + 0.5) / sea_mask.shape[0]
    coriolis = jnp.sin(latitude)[:, None]
    east_new = sea_tile * (
        centre[0]
        + OCEAN_STEP * (coriolis * (centre[1] + stokes[1]) + VISCOSITY * laplace[0] - DRAG * centre[0])
    )
    north_new = sea_tile * (
        centre[1]
        + OCEAN_STEP * (-coriolis * (centre[0] + stokes[0]) + VISCOSITY * laplace[1] - DRAG * centre[1])
    )
    return (spectrum_out, jnp.stack([east_new, north_new]))


def parts_of(group, groups, lane_tiles):
    size = lane_tiles // BLOCKS
    return [size, lane_tiles - size] if group == groups - 1 else [lane_tiles]


def fits(mesh, spectrum):
    comps, rows_all, width = spectrum.shape
    count = mesh.shape["comp"]
    return (
        (comps // count) % DIRS == 0
        and count & (count - 1) == 0
        and rows_all // mesh.shape["band"] == SUBLANES
        and width % (count * BLOCKS * LANES) == 0
    )


def solution(mesh):
    in_specs = (P("comp", "band", None), P(None, "band", "comp"), P(), P(), P(), P(), P(), P())
    out_specs = (P("comp", "band", None), P(None, "band", "comp"))
    shard = functools.partial(jax.shard_map, mesh=mesh, in_specs=in_specs, out_specs=out_specs, check_vma=False)

    def step(spectrum, *others):
        if not fits(mesh, spectrum):
            return shard(local)(spectrum, *others)

        return shard(local_fused)(spectrum, *others)

    return step
```
